32 devices in a mesh: samp: 4 (over x, core), snp: 8 (over z, y).
Axes of the slice: x: 2, y: 2, z: 4, core: 2. Of those that a mesh axis runs over, the one named last changes fastest.
Arguments:
- genotype: bfloat16 [40960, 40960], P('samp', 'snp'), may hold values from 0 to 2, as said below
- centre: float32 [40960], P('snp'), may hold values from 0.1 to 1
- spread: float32 [40960], P('snp'), may hold values from 0.308 to 0.7072
- pheno_probes: float32 [32, 40960], P(None, ('samp', 'snp')), may hold values from -15.75 to 15.75
Outputs:
- solution: float32 [32, 40960], P(None, ('samp', 'snp'))
- marker_stats: float32 [32, 40960], P(None, 'snp')
The draws below stay inside these ranges and needn't reach their ends.
Inputs may be any that keep to these rules, and one draw needn't show every extreme that they name: `genotype`: whole numbers.
All inputs are finite; a program needn't handle non-finite values.
Results may differ from the reference program's by a relative error of at most 0.0003.
Values sent between devices are 32-bit elements; how exact they have to be, the bound alone decides.
A program may use at most 448 MiB of HBM per device.

```python
import math
import jax
import jax.numpy as jnp
from jax import lax

SAMPLES = 40960
MARKERS = 40960
PROBES = 32
ROUNDS = 3
N_SNP = 8


def allele_rate(key):
    return jax.random.randint(jax.random.fold_in(key, 11), (MARKERS,), 50, 501)


def draw_genotype(key, part):
    rates = allele_rate(key)
    coded = jax.random.randint(jax.random.fold_in(key, 23), (SAMPLES, MARKERS), 0, 1000000)
    leading_replica = (coded % 1000 < rates[None, :]).astype(jnp.int32)
    second_copy = (coded // 1000 < rates[None, :]).astype(jnp.int32)
    return (leading_replica + second_copy).astype(jnp.float32).astype(jnp.bfloat16)


def draw_centre(key, part):
    rates = allele_rate(key).astype(jnp.float32) / 1000.0
    return 2.0 * rates


def draw_spread(key, part):
    rates = allele_rate(key).astype(jnp.float32) / 1000.0
    return jnp.sqrt(2.0 * rates * (1.0 - rates))


def draw_pheno_probes(key, part):
    position = jnp.arange(SAMPLES, dtype=jnp.float32) / (SAMPLES - 1)
    noise = jnp.clip(jax.random.normal(jax.random.fold_in(key, 31), (PROBES, SAMPLES), jnp.float32), -4.0, 4.0)
    return noise * (1.0 + 2.0 * position)[None, :]


def setup_inputs(seed: int = 0) -> dict:
    arg_keys = jax.random.split(jax.random.key(seed), 5)
    genotype = draw_genotype(jax.random.fold_in(arg_keys[4], 71), 0)
    centre = draw_centre(jax.random.fold_in(arg_keys[4], 71), 0)
    spread = draw_spread(jax.random.fold_in(arg_keys[4], 71), 0)
    pheno_probes = draw_pheno_probes(jax.random.fold_in(arg_keys[4], 71), 0)
    return {"genotype": genotype, "centre": centre, "spread": spread, "pheno_probes": pheno_probes}


ridge = 0.1
exact = lax.Precision.HIGHEST

def block_scores(genotype, centre, spread, first, width):
    columns = lax.dynamic_slice_in_dim(genotype, first, width, 1)
    middles = lax.dynamic_slice_in_dim(centre, first, width, 0)
    deviations = lax.dynamic_slice_in_dim(spread, first, width, 0)
    return (columns.astype(jnp.float32) - middles[None, :]) / deviations[None, :]

def operate(vector, genotype, centre, spread):
    width = MARKERS // N_SNP

    def add_block(index, running):
        first = (index * width).astype(jnp.int32)
        scores = block_scores(genotype, centre, spread, first, width)
        marker_load = jnp.dot(vector, scores, precision=exact, preferred_element_type=jnp.float32)
        return running + lax.dot_general(marker_load, scores, (((1,), (1,)), ((), ())), precision=exact, preferred_element_type=jnp.float32)
    summed = lax.fori_loop(jnp.int32(0), jnp.int32(N_SNP), add_block, jnp.zeros(vector.shape, jnp.float32))
    return summed / MARKERS + ridge * vector

def association(solution, genotype, centre, spread):
    width = MARKERS // N_SNP

    def one_block(index, running):
        first = (index * width).astype(jnp.int32)
        scores = block_scores(genotype, centre, spread, first, width)
        marker_load = jnp.dot(solution, scores, precision=exact, preferred_element_type=jnp.float32)
        return lax.dynamic_update_slice_in_dim(running, marker_load, first, 1)
    gathered = lax.fori_loop(jnp.int32(0), jnp.int32(N_SNP), one_block, jnp.zeros((PROBES, MARKERS), jnp.float32))
    return gathered / math.sqrt(SAMPLES)

def reference(genotype, centre, spread, pheno_probes):
    solution = jnp.zeros_like(pheno_probes)
    residual = pheno_probes
    direction = pheno_probes
    norm_now = lax.optimization_barrier(jnp.sum(residual * residual, axis=1, keepdims=True))
    for counter in range(ROUNDS):
        applied = operate(direction, genotype, centre, spread)
        step_size = norm_now / lax.optimization_barrier(jnp.sum(direction * applied, axis=1, keepdims=True))
        solution = solution + step_size * direction
        residual = residual - step_size * applied
        norm_next = lax.optimization_barrier(jnp.sum(residual * residual, axis=1, keepdims=True))
        direction = residual + norm_next / norm_now * direction
        norm_now = norm_next
    return (solution, association(solution, genotype, centre, spread))
```

```python
import functools
import math

import jax
import jax.numpy as jnp
from jax import lax
from jax.experimental import pallas as pl
from jax.experimental.pallas import tpu as pltpu
from jax.sharding import PartitionSpec as P

ROUNDS = 3
RIDGE = 0.1
LANES = 128


def split(values):
    high = lax.reduce_precision(values, 8, 7)
    low = lax.reduce_precision(values - high, 8, 7)
    return jnp.concatenate([high, low], axis=0).astype(jnp.bfloat16), high + low


def product(pieces, genotype, dimension):
    rows = pieces.shape[0] // 2
    pieces = lax.dot_general(
        pieces,
        genotype,
        (((1,), (dimension,)), ((), ())),
        preferred_element_type=jnp.float32,
    )
    return pieces[:rows] + pieces[rows:]


def row_sum(values):
    return jnp.sum(values, axis=1, keepdims=True)


def with_scalars(values, scalars):
    rows = values.shape[0]
    filler = jnp.zeros((rows, LANES - len(scalars)), jnp.float32)
    return jnp.concatenate([values, *scalars, filler], axis=1)


def local(samples, markers, genotype, centre, spread, pheno_probes):
    shard = pheno_probes.shape[1]
    columns = genotype.shape[1]
    block = genotype.shape[0]
    first = lax.axis_index("snp") * shard
    inverse = 1.0 / spread[None, :]
    middle = centre[None, :]

    residual = lax.all_gather(pheno_probes, "snp", axis=1, tiled=True)
    direction = load = norm = square = None
    solution = stats = None
    for counter in range(ROUNDS):
        pieces, rounded = split(residual)
        scalars = [row_sum(rounded), row_sum(residual * residual)]
        if counter:
            scalars.append(row_sum(residual * direction))
        raw = product(pieces, genotype, 0)
        total = lax.psum(with_scalars(raw, scalars), "samp")
        residual_load = (total[:, :columns] - total[:, columns : columns + 1] * middle) * inverse
        norm_next = total[:, columns + 1 : columns + 2]
        if counter:
            ratio = norm_next / norm
            cross = total[:, columns + 2 : columns + 3]
            load = residual_load + ratio * load
            direction = residual + ratio * direction
            square = norm_next + 2.0 * ratio * cross + ratio * ratio * square
        else:
            load, direction, square = residual_load, residual, norm_next
        norm = norm_next

        power = row_sum(load * load)
        if counter < ROUNDS - 1:
            pieces, rounded = split(load * inverse)
            image = product(pieces, genotype, 1) - row_sum(rounded * middle)
            summed = lax.psum(with_scalars(image, [power]), "snp")
            power = summed[:, block : block + 1]
        else:
            power = lax.psum(power, "snp")
        step = norm / (power / markers + RIDGE * square)
        own = lax.dynamic_slice_in_dim(direction, first, shard, 1)
        solution = step * own if solution is None else solution + step * own
        stats = step * load if stats is None else stats + step * load
        if counter < ROUNDS - 1:
            applied = summed[:, :block] / markers + RIDGE * direction
            residual = residual - step * applied
    return (solution, stats / math.sqrt(samples))


MESH = pl.DeviceIdType.MESH
STORED = jnp.float8_e4m3fn
SLOTS = 7
FETCHED = 64
VMEM_LIMIT = 67043328


def swap(index, distance, count):
    result, bit = 0, 1
    while bit < count:
        result = result + bit * lax.rem(index // bit + distance // bit, 2)
        bit *= 2
    return result


def pieces_of(values):
    high = values.astype(jnp.bfloat16)
    wide = high.astype(jnp.float32)
    low = (values - wide).astype(jnp.bfloat16)
    return high, low, wide + low.astype(jnp.float32)


def lanes_sum(values):
    total = values[:, :LANES]
    for start in range(LANES, values.shape[1], LANES):
        total = total + values[:, start : start + LANES]
    return total


def solve(
    plan,
    genotype,
    centre,
    spread,
    pheno,
    solution,
    stats,
    stored,
    stage,
    pieces,
    shards,
    sent,
    paired,
    gathered,
    own_image,
    loads,
    crossed,
    faced,
    direction,
    power_sent,
    power_got,
    stage_sem,
    ag_send,
    ag_recv,
    y_send,
    y_recv,
    z_send,
    z_recv,
    c_send,
    c_recv,
    x_send,
    x_recv,
    lg_send,
    lg_recv,
    p_send,
    p_recv,
):
    samples, markers, faces, columns = plan
    root = math.sqrt(samples)
    rows = pheno.shape[0]
    width = pheno.shape[1]
    part = columns // (2 * faces)
    depth = shards.shape[0] // 2
    block_rows = stage.shape[1]
    samp, snp = lax.axis_index("samp"), lax.axis_index("snp")
    x, core = samp // 2, lax.rem(samp, 2)
    z, y = snp // 2, lax.rem(snp, 2)

    def to_snp(zz, yy):
        return (samp, zz * 2 + yy)

    def to_samp(xx, cc):
        return (xx * 2 + cc, snp)

    def remote(source, target, send, recv, device):
        return pltpu.make_async_remote_copy(
            src_ref=source,
            dst_ref=target,
            send_sem=send,
            recv_sem=recv,
            device_id=device,
            device_id_type=MESH,
        )

    def at(slot):
        return pl.multiple_of(slot * width, LANES)

    def column(slot):
        return pl.ds(pl.multiple_of(slot * part, LANES), part)

    def row_range(slot):
        return pl.ds(at(slot), width)

    lane = lax.broadcasted_iota(jnp.int32, (rows, LANES), 1)

    def packed(*scalars):
        block = jnp.zeros((rows, LANES), jnp.float32)
        for position, scalar in enumerate(scalars):
            block = jnp.where(lane == position, scalar, block)
        return block

    shards[snp, :, :width] = pheno[...]
    shards[snp, :, width:] = jnp.zeros((rows, LANES), jnp.float32)

    barrier = pltpu.get_barrier_semaphore()
    partners = [to_snp(z, 1 - y), to_samp(x, 1 - core)]
    partners += [to_snp(swap(z, d, depth), y) for d in range(1, depth)]
    partners += [to_samp(swap(x, d, faces), core) for d in range(1, faces)]
    for partner in partners:
        pl.semaphore_signal(barrier, inc=1, device_id=partner, device_id_type=MESH)

    per = width // block_rows
    blocks = 2 * depth * per

    def shard_at(step):
        return swap(z, lax.rem(step, depth), depth) * 2 + lax.rem(y + step // depth, 2)

    def fetch(index):
        slot = lax.rem(index, SLOTS)
        first = shard_at(index // per) * width + lax.rem(index, per) * block_rows
        return pltpu.make_async_copy(
            genotype.at[pl.ds(pl.multiple_of(first, block_rows), block_rows)],
            stage.at[slot],
            stage_sem.at[slot],
        )

    for index in range(SLOTS - 1):
        fetch(jnp.int32(index)).start()
    pl.semaphore_wait(barrier, len(partners))

    def own_shard_to(d):
        device = to_snp(swap(z, d, depth), y) if d else to_snp(z, 1 - y)
        return remote(shards.at[snp], shards.at[snp], ag_send.at[d], ag_recv.at[snp], device)

    def forward(d):
        slot = swap(z, d, depth) * 2 + y
        return remote(
            shards.at[slot], shards.at[slot], ag_send.at[depth + d], ag_recv.at[slot], to_snp(z, 1 - y)
        )

    def shard_arrival(slot):
        return remote(shards.at[slot], shards.at[slot], ag_send.at[0], ag_recv.at[slot], to_snp(z, 1 - y))

    def load_stored(step):
        def one(q, carry):
            index = step * per + q

            @pl.when(index + SLOTS - 1 < blocks)
            def _():
                fetch(index + SLOTS - 1).start()

            fetch(index).wait()
            first = shard_at(step) * width + q * block_rows
            where = pl.ds(pl.multiple_of(first, block_rows), block_rows)
            stored[where, :] = stage[lax.rem(index, SLOTS)].astype(STORED)
            return carry

        lax.fori_loop(0, per, one, 0)

    def receive_shard(step):
        @pl.when(step > 0)
        def _():
            shard_arrival(shard_at(step)).wait_recv()

        @pl.when(jnp.logical_and(step > 0, step < depth))
        def _():
            forward(step).start()

    def take_shard(slot, sums):
        values = shards[slot, :, :width]
        high, low, rounded = pieces_of(values)
        pieces[slot, :rows, :width] = high
        pieces[slot, rows:, :width] = low
        return (
            sums[0] + lanes_sum(rounded),
            sums[1] + lanes_sum(values * values),
            sums[2] + shards[slot, :, width:],
        )

    def raw_part(slot, target):
        result = jnp.dot(
            pieces[slot, :, :width],
            stored[row_range(slot), column(target)],
            preferred_element_type=jnp.float32,
        )
        sent[target, :, :part] += result[:rows] + result[rows:]

    def core_send(xx):
        return remote(
            sent.at[xx * 2 + 1 - core], crossed.at[xx], c_send.at[xx], c_recv.at[xx], to_samp(x, 1 - core)
        )

    def face_send(xx):
        return remote(crossed.at[xx], faced.at[x], x_send.at[xx], x_recv.at[x], to_samp(xx, core))

    def face_arrival(xx):
        return remote(crossed.at[xx], faced.at[xx], x_send.at[xx], x_recv.at[xx], to_samp(xx, core))

    def own_load_to(d):
        device = to_samp(swap(x, d, faces), core) if d else to_samp(x, 1 - core)
        return remote(loads.at[samp], loads.at[samp], lg_send.at[d], lg_recv.at[samp], device)

    def load_forward(d):
        slot = swap(x, d, faces) * 2 + core
        return remote(
            loads.at[slot], loads.at[slot], lg_send.at[faces + d], lg_recv.at[slot], to_samp(x, 1 - core)
        )

    def load_arrival(slot):
        return remote(loads.at[slot], loads.at[slot], lg_send.at[0], lg_recv.at[slot], to_samp(x, 1 - core))

    def take_load(slot, sums):
        values = loads[slot]
        high, low, rounded = pieces_of(values * (1.0 / spread[:, column(slot)]))
        pieces[slot, :rows, :part] = high
        pieces[slot, rows:, :part] = low
        return (
            sums[0] + lanes_sum(rounded * centre[:, column(slot)]),
            sums[1] + lanes_sum(values * values),
        )

    def image_part(slot):
        result = None
        for source in range(2 * faces):
            term = lax.dot_general(
                pieces[source, :, :part],
                stored[row_range(slot), source * part : (source + 1) * part],
                (((1,), (1,)), ((), ())),
                preferred_element_type=jnp.float32,
            )
            result = term if result is None else result + term
        return result[:rows] + result[rows:]

    def pair_send(zz):
        return remote(sent.at[zz], paired.at[zz], y_send.at[zz], y_recv.at[zz], to_snp(z, 1 - y))

    def far_send(zz):
        return remote(paired.at[zz], gathered.at[z], z_send.at[zz], z_recv.at[z], to_snp(zz, y))

    def far_arrival(zz):
        return remote(paired.at[zz], gathered.at[zz], z_send.at[zz], z_recv.at[zz], to_snp(zz, y))

    norm = square = None
    for counter in range(ROUNDS):
        for d in range(depth):
            own_shard_to(d).start()
        if counter:
            for slot in range(2 * faces):
                where = slice(slot * part, (slot + 1) * part)
                update = step * loads[slot]
                stats[:, where] = update if counter == 1 else stats[:, where] + update
        sent[...] = jnp.zeros(sent.shape, jnp.float32)

        def one_shard(index, sums, counter=counter):
            if not counter:
                load_stored(index)
            receive_shard(index)
            slot = shard_at(index)
            sums = take_shard(slot, sums)

            def one_part(target, carry):
                raw_part(slot, target)
                return carry

            lax.fori_loop(0, 2 * faces, one_part, 0)
            return sums

        empty = jnp.zeros((rows, LANES), jnp.float32)
        last = 2 * depth - 1
        sums = lax.fori_loop(0, last, one_shard, (empty, empty, empty))
        if not counter:
            load_stored(last)
        slot = shard_at(last)
        shard_arrival(slot).wait_recv()
        sums = take_shard(slot, sums)
        scalars = packed(row_sum(sums[0]), row_sum(sums[1]), sums[2][:, :1])
        for target in range(2 * faces):
            sent[target, :, part:] = scalars
        order = [swap(x, d, faces) for d in range(faces - 1, -1, -1)]
        for xx in order:
            raw_part(slot, xx * 2 + 1 - core)
            core_send(xx).start()
        for xx in order:
            raw_part(slot, xx * 2 + core)
        for xx in order[:-1]:
            core_send(xx).wait_recv()
            crossed[xx] += sent[xx * 2 + core]
            face_send(xx).start()
        core_send(x).wait_recv()
        total = crossed[x] + sent[samp]
        for xx in order[:-1]:
            face_arrival(xx).wait_recv()
            total = total + faced[xx]

        norm_next = total[:, part + 1 : part + 2]
        load = (total[:, :part] - total[:, part : part + 1] * centre[:, column(samp)]) * (
            1.0 / spread[:, column(samp)]
        )
        if counter:
            ratio = norm_next / norm
            cross = total[:, part + 2 : part + 3]
            load = load + ratio * loads[samp]
            square = norm_next + 2.0 * ratio * cross + ratio * ratio * square
            loads[samp] = load
        else:
            square = norm_next
            loads[samp] = load
        for xx in order[:-1]:
            face_send(xx).wait_send()
        for d in range(depth):
            own_shard_to(d).wait_send()
        for d in range(1, depth):
            forward(d).wait_send()
        for d in range(faces - 1, -1, -1):
            own_load_to(d).start()
        if counter:
            direction[...] = shards[snp, :, :width] + ratio * direction[...]
        else:
            direction[...] = shards[snp, :, :width]
        norm = norm_next

        sums = take_load(samp, (empty, empty))
        for d in range(1, faces):
            other = swap(x, d, faces) * 2 + core
            load_arrival(other).wait_recv()
            load_forward(d).start()
            sums = take_load(other, sums)
        for d in range(faces):
            other = swap(x, d, faces) * 2 + 1 - core
            load_arrival(other).wait_recv()
            sums = take_load(other, sums)
        power = row_sum(sums[1])

        if counter < ROUNDS - 1:
            offset = row_sum(sums[0])
            scalars = packed(power)
            for xx in order:
                core_send(xx).wait_send()

            def one_image(index, carry, offset=offset, scalars=scalars):
                own = jnp.logical_or(
                    index == 2 * depth - 1, jnp.logical_and(index > 0, lax.rem(index, 2) == 0)
                )
                ahead = jnp.where(index == 2 * depth - 1, depth - 1, (index + 1) // 2)
                rank = jnp.where(
                    jnp.logical_and(index < 2 * depth - 1, own), index // 2 - 1, ahead
                )
                zz = swap(z, depth - 1 - rank, depth)
                slot = zz * 2 + jnp.where(own, y, 1 - y)
                own_image[...] = image_part(slot) - offset

                @pl.when(jnp.logical_not(own))
                def _():
                    sent[zz, :, :width] = own_image[...]
                    sent[zz, :, width:] = scalars
                    pair_send(zz).start()

                @pl.when(own)
                def _():
                    pair_send(zz).wait_recv()
                    paired[zz, :, :width] += own_image[...]
                    paired[zz, :, width:] += scalars

                @pl.when(jnp.logical_and(own, index < 2 * depth - 1))
                def _():
                    far_send(zz).start()

                return carry

            lax.fori_loop(0, 2 * depth, one_image, 0)
            total = paired[z]
            for d in range(depth - 1, 0, -1):
                zz = swap(z, d, depth)
                far_arrival(zz).wait_recv()
                total = total + gathered[zz]
            power = total[:, width : width + 1]
            step = norm / (power / markers + RIDGE * square)
            own_direction = direction[...]
            update = step * own_direction
            applied = total[:, :width] / markers + RIDGE * own_direction
            residual = shards[snp, :, :width] - step * applied
            shards[snp, :, :width] = residual
            shards[snp, :, width:] = packed(row_sum(residual * own_direction))
            solution[...] = update if not counter else solution[...] + update
            for d in range(depth):
                pair_send(swap(z, d, depth)).wait_send()
            for d in range(1, depth):
                far_send(swap(z, d, depth)).wait_send()
        else:
            power_sent[0] = jnp.broadcast_to(power, (rows, LANES))
            swap_power = remote(
                power_sent.at[0], power_got.at[z], p_send.at[0], p_recv.at[z], to_snp(z, 1 - y)
            )
            swap_power.start()
            swap_power.wait_recv()
            power_sent[1] = power_sent[0] + power_got[z]
            total = power_sent[1]

            def spread_power(d, source):
                return remote(
                    power_sent.at[1],
                    power_got.at[source],
                    p_send.at[d],
                    p_recv.at[source],
                    to_snp(swap(z, d, depth), y),
                )

            for d in range(1, depth):
                spread_power(d, z).start()
            for d in range(1, depth):
                source = swap(z, d, depth)
                spread_power(d, source).wait_recv()
                total = total + power_got[source]
            step = norm / (total[:, :1] / markers + RIDGE * square)
            solution[...] += step * direction[...]
            for slot in range(2 * faces):
                where = slice(slot * part, (slot + 1) * part)
                stats[:, where] = (stats[:, where] + step * loads[slot]) / root
            swap_power.wait_send()
            for d in range(1, depth):
                spread_power(d, z).wait_send()
            for xx in order:
                core_send(xx).wait_send()
        for d in range(faces):
            own_load_to(d).wait_send()
        for d in range(1, faces):
            load_forward(d).wait_send()


def power_of_two(count):
    return count > 0 and count & (count - 1) == 0


def fits(mesh, genotype, pheno_probes):
    groups, sections = mesh.shape["samp"], mesh.shape["snp"]
    if groups % 2 or sections % 2 or not power_of_two(groups) or not power_of_two(sections):
        return False
    samples, markers = genotype.shape
    rows = pheno_probes.shape[0]
    block, columns = samples // groups, markers // sections
    width, part = block // sections, columns // groups
    if rows % 16 or width % LANES or width != part or sections // 2 < groups or groups < 4:
        return False
    shard = rows * (width + LANES) * 4
    used = block * columns + SLOTS * FETCHED * columns * 2 + sections * rows * width * 4
    used += (sections + 3 * sections // 2 + 2 * groups + 6) * shard
    return used < VMEM_LIMIT


def resident(samples, markers, groups, sections, genotype, centre, spread, pheno_probes):
    rows, width = pheno_probes.shape
    block, columns = genotype.shape
    faces, depth = groups // 2, sections // 2
    part = columns // groups
    message = (rows, width + LANES)
    f32 = jnp.float32
    dma = pltpu.SemaphoreType.DMA
    flops = 2 * (2 * ROUNDS - 1) * 2 * rows * block * columns
    return pl.pallas_call(
        functools.partial(solve, (samples, markers, faces, columns)),
        out_shape=(
            jax.ShapeDtypeStruct((rows, width), f32),
            jax.ShapeDtypeStruct((rows, columns), f32),
        ),
        in_specs=[pl.BlockSpec(memory_space=pl.ANY)] + [pl.BlockSpec(memory_space=pltpu.VMEM)] * 3,
        out_specs=[pl.BlockSpec(memory_space=pltpu.VMEM)] * 2,
        scratch_shapes=[
            pltpu.VMEM((block, columns), STORED),
            pltpu.VMEM((SLOTS, FETCHED, columns), jnp.bfloat16),
            pltpu.VMEM((sections, 2 * rows, width), jnp.bfloat16),
            pltpu.VMEM((sections, *message), f32),
            pltpu.VMEM((max(groups, depth), *message), f32),
            pltpu.VMEM((depth, *message), f32),
            pltpu.VMEM((depth, *message), f32),
            pltpu.VMEM((rows, width), f32),
            pltpu.VMEM((groups, rows, part), f32),
            pltpu.VMEM((faces, *message), f32),
            pltpu.VMEM((faces, *message), f32),
            pltpu.VMEM((rows, width), f32),
            pltpu.VMEM((2, rows, LANES), f32),
            pltpu.VMEM((depth, rows, LANES), f32),
            dma((SLOTS,)),
            dma((2 * depth,)),
            dma((sections,)),
            dma((depth,)),
            dma((depth,)),
            dma((depth,)),
            dma((depth,)),
            dma((faces,)),
            dma((faces,)),
            dma((faces,)),
            dma((faces,)),
            dma((2 * faces,)),
            dma((groups,)),
            dma((depth,)),
            dma((depth,)),
        ],
        compiler_params=pltpu.CompilerParams(
            collective_id=0, has_side_effects=True, vmem_limit_bytes=VMEM_LIMIT
        ),
        cost_estimate=pl.CostEstimate(
            flops=flops, bytes_accessed=2 * block * columns, transcendentals=0
        ),
    )(genotype, centre[None, :], spread[None, :], pheno_probes)


def solution(mesh):
    in_specs = (P("samp", "snp"), P("snp"), P("snp"), P(None, ("samp", "snp")))
    out_specs = (P(None, ("samp", "snp")), P(None, "snp"))

    def whole(genotype, centre, spread, pheno_probes):
        samples, markers = genotype.shape

        def body(*blocks):
            if fits(mesh, genotype, pheno_probes):
                sizes = (samples, markers, mesh.shape["samp"], mesh.shape["snp"])
                return resident(*sizes, *blocks)
            return local(samples, markers, *blocks)

        return jax.shard_map(
            body, mesh=mesh, in_specs=in_specs, out_specs=out_specs, check_vma=False
        )(genotype, centre, spread, pheno_probes)

    return whole
```

```python
import functools
import math

import jax
import jax.numpy as jnp
from jax import lax
from jax.experimental import pallas as pl
from jax.experimental.pallas import tpu as pltpu
from jax.sharding import PartitionSpec as P

ROUNDS = 3
RIDGE = 0.1
LANES = 128


def split(values):
    high = lax.reduce_precision(values, 8, 7)
    low = lax.reduce_precision(values - high, 8, 7)
    return jnp.concatenate([high, low], axis=0).astype(jnp.bfloat16), high + low


def product(pieces, genotype, dimension):
    rows = pieces.shape[0] // 2
    pieces = lax.dot_general(
        pieces,
        genotype,
        (((1,), (dimension,)), ((), ())),
        preferred_element_type=jnp.float32,
    )
    return pieces[:rows] + pieces[rows:]


def row_sum(values):
    return jnp.sum(values, axis=1, keepdims=True)


def with_scalars(values, scalars):
    rows = values.shape[0]
    filler = jnp.zeros((rows, LANES - len(scalars)), jnp.float32)
    return jnp.concatenate([values, *scalars, filler], axis=1)


def local(samples, markers, genotype, centre, spread, pheno_probes):
    shard = pheno_probes.shape[1]
    columns = genotype.shape[1]
    block = genotype.shape[0]
    first = lax.axis_index("snp") * shard
    inverse = 1.0 / spread[None, :]
    middle = centre[None, :]

    residual = lax.all_gather(pheno_probes, "snp", axis=1, tiled=True)
    direction = load = norm = square = None
    solution = stats = None
    for counter in range(ROUNDS):
        pieces, rounded = split(residual)
        scalars = [row_sum(rounded), row_sum(residual * residual)]
        if counter:
            scalars.append(row_sum(residual * direction))
        raw = product(pieces, genotype, 0)
        total = lax.psum(with_scalars(raw, scalars), "samp")
        residual_load = (total[:, :columns] - total[:, columns : columns + 1] * middle) * inverse
        norm_next = total[:, columns + 1 : columns + 2]
        if counter:
            ratio = norm_next / norm
            cross = total[:, columns + 2 : columns + 3]
            load = residual_load + ratio * load
            direction = residual + ratio * direction
            square = norm_next + 2.0 * ratio * cross + ratio * ratio * square
        else:
            load, direction, square = residual_load, residual, norm_next
        norm = norm_next

        power = row_sum(load * load)
        if counter < ROUNDS - 1:
            pieces, rounded = split(load * inverse)
            image = product(pieces, genotype, 1) - row_sum(rounded * middle)
            summed = lax.psum(with_scalars(image, [power]), "snp")
            power = summed[:, block : block + 1]
        else:
            power = lax.psum(power, "snp")
        step = norm / (power / markers + RIDGE * square)
        own = lax.dynamic_slice_in_dim(direction, first, shard, 1)
        solution = step * own if solution is None else solution + step * own
        stats = step * load if stats is None else stats + step * load
        if counter < ROUNDS - 1:
            applied = summed[:, :block] / markers + RIDGE * direction
            residual = residual - step * applied
    return (solution, stats / math.sqrt(samples))


MESH = pl.DeviceIdType.MESH
STORED = jnp.float8_e4m3fn
SUBLANES = 8
FACING = 4
SLOTS = 7
FETCHED = 64
VMEM_LIMIT = 67043328


def swap(index, distance, count):
    result, bit = 0, 1
    while bit < count:
        result = result + bit * lax.rem(index // bit + distance // bit, 2)
        bit *= 2
    return result


def pieces_of(values):
    high = values.astype(jnp.bfloat16)
    wide = high.astype(jnp.float32)
    low = (values - wide).astype(jnp.bfloat16)
    return high, low, wide + low.astype(jnp.float32)


def read(ref, slot, rows):
    blocks = (ref.shape[1] - SUBLANES) // rows
    return jnp.concatenate([ref[slot, q * rows : (q + 1) * rows, :] for q in range(blocks)], axis=1)


def write(ref, slot, values):
    rows = values.shape[0]
    for q in range(values.shape[1] // LANES):
        ref[slot, q * rows : (q + 1) * rows, :] = values[:, q * LANES : (q + 1) * LANES]


def tail_of(ref):
    return pl.ds(ref.shape[1] - SUBLANES, SUBLANES)


def lanes_sum(values):
    total = values[:, :LANES]
    for start in range(LANES, values.shape[1], LANES):
        total = total + values[:, start : start + LANES]
    return total


def solve(
    plan,
    genotype,
    centre,
    spread,
    pheno,
    solution,
    stats,
    stored,
    stage,
    pieces,
    shards,
    sent,
    paired,
    gathered,
    own_image,
    loads,
    crossed,
    faced,
    direction,
    power_sent,
    power_got,
    stage_sem,
    ag_send,
    ag_recv,
    y_send,
    y_recv,
    z_send,
    z_recv,
    c_send,
    c_recv,
    x_send,
    x_recv,
    lg_send,
    lg_recv,
    p_send,
    p_recv,
):
    samples, markers, faces, columns = plan
    root = math.sqrt(samples)
    rows = pheno.shape[0]
    width = pheno.shape[1]
    part = columns // (2 * faces)
    depth = shards.shape[0] // 2
    block_rows = stage.shape[1]
    samp, snp = lax.axis_index("samp"), lax.axis_index("snp")
    x, core = samp // 2, lax.rem(samp, 2)
    z, y = snp // 2, lax.rem(snp, 2)

    def to_snp(zz, yy):
        return (samp, zz * 2 + yy)

    def to_samp(xx, cc):
        return (xx * 2 + cc, snp)

    def remote(source, target, send, recv, device):
        return pltpu.make_async_remote_copy(
            src_ref=source,
            dst_ref=target,
            send_sem=send,
            recv_sem=recv,
            device_id=device,
            device_id_type=MESH,
        )

    def at(slot):
        return pl.multiple_of(slot * width, LANES)

    def column(slot):
        return pl.ds(pl.multiple_of(slot * part, LANES), part)

    def row_range(slot):
        return pl.ds(at(slot), width)

    lane = lax.broadcasted_iota(jnp.int32, (rows, LANES), 1)
    diagonal = lane == lax.broadcasted_iota(jnp.int32, (rows, LANES), 0)
    line = lax.broadcasted_iota(jnp.int32, (SUBLANES, LANES), 0)
    nothing = jnp.zeros((SUBLANES, LANES), jnp.float32)

    def packed(*scalars):
        tile = nothing
        for position, scalar in enumerate(scalars):
            turned = jnp.sum(jnp.where(diagonal, scalar, 0.0), axis=0, keepdims=True)
            tile = jnp.where(line == position, turned, tile)
        return tile

    def unpacked(tile, position):
        return row_sum(jnp.where(diagonal, tile[position : position + 1, :], 0.0))

    write(shards, snp, pheno[...])
    tail = tail_of(shards)
    shards[snp, tail, :] = nothing

    barrier = pltpu.get_barrier_semaphore()
    partners = [to_snp(z, 1 - y), to_samp(x, 1 - core)]
    partners += [to_snp(swap(z, d, depth), y) for d in range(1, depth)]
    partners.append(to_samp(1 - x, core))
    for partner in partners:
        pl.semaphore_signal(barrier, inc=1, device_id=partner, device_id_type=MESH)

    per = width // block_rows
    blocks = 2 * depth * per

    def step_of(turn):
        later = jnp.where(turn > depth, turn, turn - 1)
        return jnp.where(turn < 2, turn, jnp.where(turn == 2, depth, later))

    def shard_at(turn):
        step = step_of(turn)
        return swap(z, lax.rem(step, depth), depth) * 2 + lax.rem(y + step // depth, 2)

    def fetch(index):
        slot = lax.rem(index, SLOTS)
        first = shard_at(index // per) * width + lax.rem(index, per) * block_rows
        return pltpu.make_async_copy(
            genotype.at[pl.ds(pl.multiple_of(first, block_rows), block_rows)],
            stage.at[slot],
            stage_sem.at[slot],
        )

    for index in range(SLOTS - 1):
        fetch(jnp.int32(index)).start()
    pl.semaphore_wait(barrier, len(partners))

    def own_shard_to(d):
        device = to_snp(swap(z, d, depth), y) if d else to_snp(z, 1 - y)
        return remote(shards.at[snp], shards.at[snp], ag_send.at[d], ag_recv.at[snp], device)

    def forward(d):
        slot = swap(z, d, depth) * 2 + y
        return remote(
            shards.at[slot], shards.at[slot], ag_send.at[depth + d], ag_recv.at[slot], to_snp(z, 1 - y)
        )

    def shard_arrival(slot):
        return remote(shards.at[slot], shards.at[slot], ag_send.at[0], ag_recv.at[slot], to_snp(z, 1 - y))

    def load_stored(step):
        def one(q, carry):
            index = step * per + q

            @pl.when(index + SLOTS - 1 < blocks)
            def _():
                fetch(index + SLOTS - 1).start()

            fetch(index).wait()
            first = shard_at(step) * width + q * block_rows
            where = pl.ds(pl.multiple_of(first, block_rows), block_rows)
            stored[where, :] = stage[lax.rem(index, SLOTS)].astype(STORED)
            return carry

        lax.fori_loop(0, per, one, 0)

    def receive_shard(turn):
        step = step_of(turn)

        @pl.when(step > 0)
        def _():
            shard_arrival(shard_at(turn)).wait_recv()

        @pl.when(jnp.logical_and(step > 0, step < depth))
        def _():
            forward(step).start()

    def take_shard(slot, sums):
        values = read(shards, slot, rows)
        high, low, rounded = pieces_of(values)
        pieces[slot, :rows, :width] = high
        pieces[slot, rows:, :width] = low
        return (
            sums[0] + lanes_sum(rounded),
            sums[1] + lanes_sum(values * values),
            sums[2] + shards[slot, tail, :],
        )

    def raw_part(slot, target):
        result = jnp.dot(
            pieces[slot, :, :width],
            stored[row_range(slot), column(target)],
            preferred_element_type=jnp.float32,
        )
        write(sent, target, read(sent, target, rows) + (result[:rows] + result[rows:]))

    def core_send(xx):
        return remote(
            sent.at[xx * 2 + 1 - core], crossed.at[xx], c_send.at[xx], c_recv.at[xx], to_samp(x, 1 - core)
        )

    def face_exchange(xx, turn):
        slot = turn * faces + xx
        return remote(
            crossed.at[xx], faced.at[slot], x_send.at[xx], x_recv.at[slot], to_samp(1 - x, core)
        )

    def load_exchange(slot):
        return remote(
            loads.at[slot], loads.at[slot], lg_send.at[slot], lg_recv.at[slot], to_samp(x, 1 - core)
        )

    def take_load(slot, sums):
        values = loads[slot]
        high, low, rounded = pieces_of(values * (1.0 / spread[:, column(slot)]))
        pieces[slot, :rows, :part] = high
        pieces[slot, rows:, :part] = low
        return (
            sums[0] + lanes_sum(rounded * centre[:, column(slot)]),
            sums[1] + lanes_sum(values * values),
        )

    def image_part(slot):
        result = None
        for source in range(2 * faces):
            term = lax.dot_general(
                pieces[source, :, :part],
                stored[row_range(slot), source * part : (source + 1) * part],
                (((1,), (1,)), ((), ())),
                preferred_element_type=jnp.float32,
            )
            result = term if result is None else result + term
        return result[:rows] + result[rows:]

    def pair_send(zz):
        return remote(sent.at[zz], paired.at[zz], y_send.at[zz], y_recv.at[zz], to_snp(z, 1 - y))

    def far_send(zz):
        return remote(paired.at[zz], gathered.at[z], z_send.at[zz], z_recv.at[z], to_snp(zz, y))

    def far_arrival(zz):
        return remote(paired.at[zz], gathered.at[zz], z_send.at[zz], z_recv.at[zz], to_snp(zz, y))

    norm = square = None
    for counter in range(ROUNDS):
        for d in range(depth):
            own_shard_to(d).start()
        if counter:
            for slot in range(2 * faces):
                where = slice(slot * part, (slot + 1) * part)
                update = step * loads[slot]
                stats[:, where] = update if counter == 1 else stats[:, where] + update
        sent[...] = jnp.zeros(sent.shape, jnp.float32)

        def one_shard(index, sums, counter=counter):
            if not counter:
                load_stored(index)
            receive_shard(index)
            slot = shard_at(index)
            sums = take_shard(slot, sums)

            def one_part(target, carry):
                raw_part(slot, target)
                return carry

            lax.fori_loop(0, 2 * faces, one_part, 0)
            return sums

        empty = jnp.zeros((rows, LANES), jnp.float32)
        last = jnp.int32(2 * depth - 1)
        sums = lax.fori_loop(0, last, one_shard, (empty, empty, nothing))
        if not counter:
            load_stored(last)
        slot = shard_at(last)
        shard_arrival(slot).wait_recv()
        sums = take_shard(slot, sums)
        scalars = packed(row_sum(sums[0]), row_sum(sums[1]), unpacked(sums[2], 0))
        for target in range(2 * faces):
            sent[target, tail, :] = scalars
        order = [1 - x, x]
        for xx in order:
            raw_part(slot, xx * 2 + 1 - core)
            core_send(xx).start()
        for xx in order:
            raw_part(slot, xx * 2 + core)
        for xx in order:
            core_send(xx).wait_recv()
            crossed[xx] += sent[xx * 2 + core]
            face_exchange(xx, counter % 2).start()
        for d in range(depth):
            own_shard_to(d).wait_send()
        for d in range(1, depth):
            forward(d).wait_send()
        sums = (empty, empty)
        norm_next = None
        for xx in order:
            arrival = face_exchange(xx, counter % 2)
            arrival.wait_recv()
            slot = xx * 2 + core
            where = faced.at[counter % 2 * faces + xx]
            if norm_next is None:
                scalars = crossed[xx, tail, :] + where[tail, :]
                offset, norm_next = unpacked(scalars, 0), unpacked(scalars, 1)
                if counter:
                    ratio = norm_next / norm
                    cross = unpacked(scalars, 2)
                    square = norm_next + 2.0 * ratio * cross + ratio * ratio * square
                else:
                    square = norm_next
            total = read(crossed, xx, rows) + read(faced, counter % 2 * faces + xx, rows)
            load = (total - offset * centre[:, column(slot)]) * (1.0 / spread[:, column(slot)])
            loads[slot] = load + ratio * loads[slot] if counter else load
            arrival.wait_send()
            load_exchange(slot).start()
            sums = take_load(slot, sums)
        if counter:
            direction[...] = read(shards, snp, rows) + ratio * direction[...]
        else:
            direction[...] = read(shards, snp, rows)
        norm = norm_next
        for xx in order:
            other = xx * 2 + 1 - core
            load_exchange(other).wait_recv()
            sums = take_load(other, sums)
        power = row_sum(sums[1])

        if counter < ROUNDS - 1:
            offset = row_sum(sums[0])
            scalars = packed(power)
            for xx in order:
                core_send(xx).wait_send()

            def one_image(index, carry, offset=offset, scalars=scalars):
                own = jnp.logical_or(
                    index == 2 * depth - 1, jnp.logical_and(index > 0, lax.rem(index, 2) == 0)
                )
                ahead = jnp.where(index == 2 * depth - 1, depth - 1, (index + 1) // 2)
                rank = jnp.where(
                    jnp.logical_and(index < 2 * depth - 1, own), index // 2 - 1, ahead
                )
                zz = swap(z, depth - 1 - rank, depth)
                slot = zz * 2 + jnp.where(own, y, 1 - y)
                own_image[...] = image_part(slot) - offset

                @pl.when(jnp.logical_not(own))
                def _():
                    write(sent, zz, own_image[...])
                    sent[zz, tail, :] = scalars
                    pair_send(zz).start()

                @pl.when(own)
                def _():
                    pair_send(zz).wait_recv()
                    write(paired, zz, read(paired, zz, rows) + own_image[...])
                    paired[zz, tail, :] += scalars

                @pl.when(jnp.logical_and(own, index < 2 * depth - 1))
                def _():
                    far_send(zz).start()

                return carry

            lax.fori_loop(0, 2 * depth, one_image, 0)
            total, scalars = read(paired, z, rows), paired[z, tail, :]
            for d in range(depth - 1, 0, -1):
                zz = swap(z, d, depth)
                far_arrival(zz).wait_recv()
                total = total + read(gathered, zz, rows)
                scalars = scalars + gathered[zz, tail, :]
            power = unpacked(scalars, 0)
            step = norm / (power / markers + RIDGE * square)
            own_direction = direction[...]
            update = step * own_direction
            applied = total / markers + RIDGE * own_direction
            residual = read(shards, snp, rows) - step * applied
            write(shards, snp, residual)
            shards[snp, tail, :] = packed(row_sum(residual * own_direction))
            solution[...] = update if not counter else solution[...] + update
            for d in range(depth):
                pair_send(swap(z, d, depth)).wait_send()
            for d in range(1, depth):
                far_send(swap(z, d, depth)).wait_send()
        else:
            power_sent[0] = jnp.broadcast_to(power, (rows, LANES))
            swap_power = remote(
                power_sent.at[0], power_got.at[z], p_send.at[0], p_recv.at[z], to_snp(z, 1 - y)
            )
            swap_power.start()
            swap_power.wait_recv()
            power_sent[1] = power_sent[0] + power_got[z]
            total = power_sent[1]

            def spread_power(d, source):
                return remote(
                    power_sent.at[1],
                    power_got.at[source],
                    p_send.at[d],
                    p_recv.at[source],
                    to_snp(swap(z, d, depth), y),
                )

            for d in range(1, depth):
                spread_power(d, z).start()
            for d in range(1, depth):
                source = swap(z, d, depth)
                spread_power(d, source).wait_recv()
                total = total + power_got[source]
            step = norm / (total[:, :1] / markers + RIDGE * square)
            solution[...] += step * direction[...]
            for slot in range(2 * faces):
                where = slice(slot * part, (slot + 1) * part)
                stats[:, where] = (stats[:, where] + step * loads[slot]) / root
            swap_power.wait_send()
            for d in range(1, depth):
                spread_power(d, z).wait_send()
            for xx in order:
                core_send(xx).wait_send()
        for xx in range(faces):
            load_exchange(xx * 2 + core).wait_send()


def power_of_two(count):
    return count > 0 and count & (count - 1) == 0


def fits(mesh, genotype, pheno_probes):
    groups, sections = mesh.shape["samp"], mesh.shape["snp"]
    if groups % 2 or sections % 2 or not power_of_two(groups) or not power_of_two(sections):
        return False
    samples, markers = genotype.shape
    rows = pheno_probes.shape[0]
    block, columns = samples // groups, markers // sections
    width, part = block // sections, columns // groups
    if rows % 16 or width % LANES or width != part or sections // 2 < groups or groups != FACING:
        return False
    shard = rows * width * 4 + SUBLANES * LANES * 4
    used = block * columns + SLOTS * FETCHED * columns * 2 + sections * rows * width * 4
    used += (sections + 3 * sections // 2 + 2 * groups + 6) * shard
    return used < VMEM_LIMIT


def resident(samples, markers, groups, sections, genotype, centre, spread, pheno_probes):
    rows, width = pheno_probes.shape
    block, columns = genotype.shape
    faces, depth = groups // 2, sections // 2
    part = columns // groups
    message = (rows * width // LANES + SUBLANES, LANES)
    f32 = jnp.float32
    dma = pltpu.SemaphoreType.DMA
    flops = 2 * (2 * ROUNDS - 1) * 2 * rows * block * columns
    return pl.pallas_call(
        functools.partial(solve, (samples, markers, faces, columns)),
        out_shape=(
            jax.ShapeDtypeStruct((rows, width), f32),
            jax.ShapeDtypeStruct((rows, columns), f32),
        ),
        in_specs=[pl.BlockSpec(memory_space=pl.ANY)] + [pl.BlockSpec(memory_space=pltpu.VMEM)] * 3,
        out_specs=[pl.BlockSpec(memory_space=pltpu.VMEM)] * 2,
        scratch_shapes=[
            pltpu.VMEM((block, columns), STORED),
            pltpu.VMEM((SLOTS, FETCHED, columns), jnp.bfloat16),
            pltpu.VMEM((sections, 2 * rows, width), jnp.bfloat16),
            pltpu.VMEM((sections, *message), f32),
            pltpu.VMEM((max(groups, depth), *message), f32),
            pltpu.VMEM((depth, *message), f32),
            pltpu.VMEM((depth, *message), f32),
            pltpu.VMEM((rows, width), f32),
            pltpu.VMEM((groups, rows, part), f32),
            pltpu.VMEM((faces, *message), f32),
            pltpu.VMEM((2 * faces, *message), f32),
            pltpu.VMEM((rows, width), f32),
            pltpu.VMEM((2, rows, LANES), f32),
            pltpu.VMEM((depth, rows, LANES), f32),
            dma((SLOTS,)),
            dma((2 * depth,)),
            dma((sections,)),
            dma((depth,)),
            dma((depth,)),
            dma((depth,)),
            dma((depth,)),
            dma((faces,)),
            dma((faces,)),
            dma((faces,)),
            dma((2 * faces,)),
            dma((groups,)),
            dma((groups,)),
            dma((depth,)),
            dma((depth,)),
        ],
        compiler_params=pltpu.CompilerParams(
            collective_id=0, has_side_effects=True, vmem_limit_bytes=VMEM_LIMIT
        ),
        cost_estimate=pl.CostEstimate(
            flops=flops, bytes_accessed=2 * block * columns, transcendentals=0
        ),
    )(genotype, centre[None, :], spread[None, :], pheno_probes)


def solution(mesh):
    in_specs = (P("samp", "snp"), P("snp"), P("snp"), P(None, ("samp", "snp")))
    out_specs = (P(None, ("samp", "snp")), P(None, "snp"))

    def whole(genotype, centre, spread, pheno_probes):
        samples, markers = genotype.shape

        def body(*blocks):
            if fits(mesh, genotype, pheno_probes):
                sizes = (samples, markers, mesh.shape["samp"], mesh.shape["snp"])
                return resident(*sizes, *blocks)
            return local(samples, markers, *blocks)

        return jax.shard_map(
            body, mesh=mesh, in_specs=in_specs, out_specs=out_specs, check_vma=False
        )(genotype, centre, spread, pheno_probes)

    return whole
```
